256 devices in a mesh: rows: 32 (over y, z), cols: 8 (over x, core).
Axes of the slice: x: 4, y: 4, z: 8, core: 2. Of those that a mesh axis runs over, the one named last changes fastest.
Arguments:
- sketches: bfloat16 [8192, 16384], P('rows', 'cols'), may hold values from -6 to 6, as said below
- start_basis: bfloat16 [16384, 256], P('cols'), may hold values from -6 to 6
- shrink_index: int32 [1], replicated, may hold values from 64 to 191
Outputs:
- shrunk: float32 [256, 16384], P('rows', 'cols')
The draws below stay inside these ranges and needn't reach their ends.
Inputs may be any that keep to these rules, and one draw needn't show every extreme that they name: `sketches`: real entries.
All inputs are finite; a program needn't handle non-finite values.
Results may differ from the reference program's by a relative error of at most 0.0028.
Values may be sent and summed in bfloat16 or wider, within the bound.
No kernel may reach another device: no remote copies, remote signals or barrier semaphores. Data moves between devices by JAX's collectives and lax.ppermute only.
A program may use at most 64 MiB of HBM per device.

```python
import math
import jax
import jax.numpy as jnp
from jax import lax

W = 16384
L = 256
ITERS = 3
STACK = 8192


def draw_sketches(key, part):
    left_key, right_key = jax.random.split(jax.random.fold_in(key, 11))
    floor_key = jax.random.fold_in(key, 17)
    column_key = jax.random.fold_in(key, 23)
    row_key = jax.random.fold_in(key, 29)
    floor_level = 0.15
    column_scales = jnp.exp(jax.random.uniform(column_key, (W,), jnp.float32, -1.0, 0.7))
    ranks = jnp.arange(L, dtype=jnp.float32)
    ratios = jnp.exp(math.log(200.0) * (1.0 - ranks / (L - 1)))
    spectrum = floor_level * jnp.sqrt(ratios / min(STACK, W))
    left_factor = jax.random.normal(left_key, (STACK, L), jnp.float32)
    right_factor = jax.random.normal(right_key, (L, W), jnp.float32)
    noise = jax.random.normal(floor_key, (STACK, W), jnp.float32)
    row_scales = jnp.exp(jax.random.uniform(row_key, (STACK,), jnp.float32, 0.0, 1.0986123))
    signal = jnp.dot(left_factor * spectrum[None, :], right_factor)
    values = (signal + floor_level * noise) * row_scales[:, None] * column_scales[None, :]
    return jnp.clip(values, -6.0, 6.0).astype(jnp.bfloat16)


def block_scale(rng, extent, pieces, low, top_value):
    gain = 1.0
    for axis_at, shards_of in pieces:
        draws = jax.random.uniform(jax.random.fold_in(jax.random.fold_in(rng, 6), axis_at), (shards_of,), jnp.float32, low / len(pieces), top_value / len(pieces))
        gain = gain * jnp.repeat(jnp.exp(draws), extent[axis_at] // shards_of).reshape((-1,) + (1,) * (len(extent) - 1 - axis_at))
    return gain


def normal_values(key, dims, deviation, most, cuts=(), kind=jnp.bfloat16):
    drawn = jax.random.normal(key, dims, jnp.float32) * deviation
    if len(cuts) > 0:
        drawn = block_scale(key, dims, cuts, -0.22, 0.18) * drawn
    return jnp.clip(drawn, min=-most, max=most).astype(kind)


def setup_inputs(seed: int = 0) -> dict:
    seeds = jax.random.split(jax.random.key(seed), 4)
    sketches = draw_sketches(jax.random.fold_in(seeds[3], 71), 0)
    start_basis = normal_values(seeds[1], (W, L), 1.0, 6.0, ((0, 8),))
    shrink_index = jax.random.randint(seeds[2], (1,), L // 4, 3 * L // 4).astype(jnp.int32)
    return {"sketches": sketches, "start_basis": start_basis, "shrink_index": shrink_index}


def orthonormal(images, gram_total):
    lower_factor = jnp.linalg.cholesky(gram_total)
    return jax.scipy.linalg.solve_triangular(lower_factor, images.T, lower=True).T

def reference(sketches, start_basis, shrink_index):
    basis_bf = start_basis
    basis = start_basis.astype(jnp.float32)
    for loop_index in range(ITERS):
        projected = jnp.dot(sketches.astype(jnp.float32), basis_bf.astype(jnp.float32), preferred_element_type=jnp.float32)
        projected_bf = projected.astype(jnp.bfloat16)
        images = jnp.dot(sketches.T.astype(jnp.float32), projected_bf.astype(jnp.float32), preferred_element_type=jnp.float32)
        gram_total = jnp.dot(images.T, images, precision=lax.Precision.HIGHEST)
        basis = orthonormal(images, gram_total)
        basis_bf = basis.astype(jnp.bfloat16)
    projected = jnp.dot(sketches.astype(jnp.float32), basis_bf.astype(jnp.float32), preferred_element_type=jnp.float32)
    energy = lax.optimization_barrier(jnp.sum(projected * projected, axis=0))
    ordered = jnp.sort(energy)[::-1]
    threshold = lax.dynamic_index_in_dim(ordered, shrink_index[0], 0, keepdims=False)
    factor = jnp.sqrt(jnp.maximum(energy - threshold, 0.25 * threshold))
    return (basis * factor[None, :]).T
```

```python
import jax
import jax.numpy as jnp
from jax import lax
from jax.experimental import pallas as pl
from jax.experimental.pallas import tpu as pltpu
from jax.sharding import Mesh, PartitionSpec as P

ITERS = 3
f32 = jnp.float32
bf16 = jnp.bfloat16
HI = lax.Precision.HIGHEST
VMEM = pl.BlockSpec(memory_space=pltpu.VMEM)
L = 256
PANEL = 32
LANES = 128


def vmem(shape, dtype=f32):
    return pltpu.VMEM(shape, dtype)


def near(*arrays):
    return tuple(pltpu.with_memory_space_constraint(x, pltpu.VMEM) for x in arrays)


def limit(mib):
    return pltpu.CompilerParams(vmem_limit_bytes=mib << 20)


def tdot(a, b):
    return lax.dot_general(a, b, (((0,), (0,)), ((), ())), precision=HI, preferred_element_type=f32)


def factor_inverse(g_ref, b_ref, w_ref, x_ref):
    sub = lax.broadcasted_iota(jnp.int32, (8, LANES), 0)
    lane = lax.broadcasted_iota(jnp.int32, (8, LANES), 1)
    groups = PANEL // 8
    b_ref[:, 0:L] = g_ref[0:LANES, :]
    b_ref[:, L:] = jnp.zeros((LANES, LANES), f32)

    def half(step, carry):
        for k in range(LANES // PANEL):
            c0 = k * PANEL
            base = b_ref[c0 : c0 + PANEL, :]
            if k > 0:
                base = base - tdot(w_ref[0:c0, c0 : c0 + PANEL], w_ref[0:c0, :])
            a = [[base[8 * q : 8 * q + 8, LANES * t : LANES * (t + 1)] for t in range(3)] for q in range(groups)]
            for q in range(groups):
                a[q][2] = a[q][2] + jnp.where(lane == sub + (c0 + 8 * q), 1.0, 0.0).astype(f32)
            for p in range(0, groups, 2):
                c = c0 + 8 * p
                col = [
                    {q: jnp.broadcast_to(a[q][0][:, c + i : c + i + 1], (8, LANES)) for q in range(p, groups)}
                    for i in range(16)
                ]
                for j in range(16):
                    h, r = p + j // 8, j % 8
                    below = range(h, groups)
                    inv = lax.rsqrt(jnp.broadcast_to(col[j][h][r : r + 1, :], (8, LANES)))
                    m = {q: col[j][q] * inv for q in below}
                    m[h] = jnp.where(sub > r, m[h], 0.0)
                    row = [jnp.broadcast_to(a[h][t][r : r + 1, :], (8, LANES)) * inv for t in range(3)]
                    for i in range(j + 1, 16):
                        ci = jnp.broadcast_to(col[i][h][r : r + 1, :], (8, LANES)) * inv
                        for q in below:
                            col[i][q] = col[i][q] - m[q] * ci
                    for q in below:
                        for t in range(3):
                            a[q][t] = a[q][t] - m[q] * row[t]
                    for t in range(3):
                        a[h][t] = jnp.where(sub == r, row[t], a[h][t])
            for q in range(groups):
                for t in range(3):
                    w_ref[c0 + 8 * q : c0 + 8 * q + 8, LANES * t : LANES * (t + 1)] = a[q][t]

        @pl.when(step == 0)
        def _():
            x_ref[0:LANES, 0:LANES] = w_ref[:, L:]
            x_ref[0:LANES, LANES:L] = jnp.zeros((LANES, LANES), f32)
            u = tdot(w_ref[:, LANES:L], w_ref[:, LANES:])
            b_ref[:, 0:LANES] = g_ref[LANES:L, LANES:L] - u[:, :LANES]
            b_ref[:, LANES:L] = -u[:, LANES:]

        @pl.when(step == 1)
        def _():
            x_ref[LANES:L, :] = w_ref[:, LANES:]

        return carry

    lax.fori_loop(0, 2, half, 0)


def step_kernel(s_ref, p_ref, x_ref, w_ref, b_ref, g_ref):
    for d in range(16):
        g_ref[16 * d : 16 * d + 16, :] = s_ref[d, 0:16, :]
    factor_inverse(g_ref, b_ref, w_ref, x_ref)
    for n in range(2):
        t = jnp.concatenate([s_ref[8 * n + d, 16:48, :] for d in range(8)], axis=0)
        p_ref[256 * n : 256 * n + 256, :] = lax.dot_general(
            t, x_ref[...], (((1,), (1,)), ((), ())), precision=HI, preferred_element_type=f32
        ).astype(p_ref.dtype)


def factor_step(s, last):
    shared = [vmem((LANES, 3 * LANES)), vmem((LANES, 3 * LANES)), vmem((L, L))]
    inverse = vmem((L, L))
    projected = vmem((512, L), f32 if last else bf16)
    return pl.pallas_call(
        step_kernel,
        out_shape=(projected, inverse) if last else projected,
        in_specs=[VMEM],
        out_specs=(VMEM, VMEM) if last else VMEM,
        scratch_shapes=shared if last else [inverse, *shared],
        compiler_params=limit(12),
        name="factor_step",
    )(*near(s))


def split(v):
    a = v.astype(bf16)
    r = v - a.astype(f32)
    b = r.astype(bf16)
    return a, b, (r - b.astype(f32)).astype(bf16)


def products_kernel(s_ref, i_ref, *refs):
    o_ref = refs[-1]
    i = i_ref[...]
    t = sum(jnp.dot(s_ref[...], part, preferred_element_type=f32) for part in split(i))
    g = tdot(i, i)
    for d in range(16):
        both = jnp.concatenate([g[16 * d : 16 * d + 16, :], t[32 * d : 32 * d + 32, :]], axis=0)
        o_ref[d] = both if len(refs) == 1 else both + refs[0][d]


def products(s, i, *add):
    return pl.pallas_call(
        products_kernel,
        out_shape=vmem((16, 48, L)),
        in_specs=[VMEM] * (2 + len(add)),
        out_specs=VMEM,
        compiler_params=limit(16),
        name="products",
    )(*near(s, i, *add))


def finish_kernel(n_ref, e_ref, a_ref, b_ref, o_ref, t_ref):
    e = e_ref[0]
    for d in range(1, 8):
        e = e + e_ref[d]
    across = jnp.broadcast_to(e, (L, L))
    t_ref[...] = jnp.transpose(across)
    down = t_ref[...]
    k = n_ref[0]
    above = jnp.sum((across > down).astype(jnp.int32), axis=1, keepdims=True)
    least = jnp.sum((across >= down).astype(jnp.int32), axis=1, keepdims=True)
    at_k = (above <= k) & (k < least)
    threshold = jnp.max(jnp.where(at_k, down[:, 0:1], -jnp.inf), axis=0, keepdims=True)
    mine = t_ref[pl.ds(pl.multiple_of(n_ref[1] * 8, 8), 8), 0:1]
    factor = jnp.sqrt(jnp.maximum(mine - threshold, 0.25 * threshold))
    odd = n_ref[2] == 1
    a = a_ref[...] * factor
    b = b_ref[...] * factor
    o_ref[:, 0:1024] = jnp.where(odd, b, a)
    o_ref[:, 1024:2048] = jnp.where(odd, a, b)


def finish(scalars, energies, a, b):
    return pl.pallas_call(
        finish_kernel,
        out_shape=jax.ShapeDtypeStruct((8, 2048), f32),
        in_specs=[pl.BlockSpec(memory_space=pltpu.SMEM)] + [VMEM] * 3,
        out_specs=VMEM,
        scratch_shapes=[pltpu.VMEM((L, L), f32)],
        compiler_params=limit(8),
        name="finish",
    )(scalars, *near(energies, a, b))


def gather(x, axis, n):
    return lax.all_to_all(jnp.broadcast_to(x, (n, *x.shape)), axis, 0, 0, tiled=True)


def scatter_sum(x, axis):
    return jnp.sum(lax.all_to_all(x, axis, 0, 0, tiled=True).astype(f32), axis=0)


def swap(x):
    return lax.ppermute(x, "c", [(0, 1), (1, 0)])


def body(sketches, start_basis, shrink_index):
    y, z, c = lax.axis_index("y"), lax.axis_index("z"), lax.axis_index("c")
    parts = []
    for k in (0, 1):
        half = lax.dynamic_slice_in_dim(sketches, ((y + k) % 2) * 1024, 1024, 1)
        pairs = [(2 * v + d, 2 * (2 * d + (v + k) % 2) + v // 2) for v in range(4) for d in range(2)]
        parts.append(lax.ppermute(half, ("y", "c"), pairs))
    odd = y % 2 == 1
    s = jnp.concatenate([jnp.where(odd, parts[1], parts[0]), jnp.where(odd, parts[0], parts[1])], axis=0)
    s_own = lax.dynamic_slice_in_dim(s, c * 512, 512, 1)
    s_oth = lax.dynamic_slice_in_dim(s, (1 - c) * 512, 512, 1)

    t = jnp.dot(sketches, start_basis, preferred_element_type=f32)
    chunk = scatter_sum(t.reshape(8, 32, L), ("x", "c")).astype(bf16)
    rows = gather(chunk, ("x", "c"), 8).reshape(256, L)
    same = lax.ppermute(rows, ("y", "c"), [(2 * v + d, 2 * (2 * (v % 2) + d) + v // 2) for v in range(4) for d in range(2)])
    flip = lax.ppermute(rows, ("y", "c"), [(2 * v + d, 2 * (2 * (1 - v % 2) + d) + v // 2) for v in range(4) for d in range(2)])
    upper = y // 2 == 1
    projected = jnp.concatenate([jnp.where(upper, flip, same), jnp.where(upper, same, flip)], axis=0)
    for it in range(ITERS):
        def images(part):
            return lax.dot_general(part, projected, (((0,), (0,)), ((), ())), preferred_element_type=f32)

        half = images(s_own) + swap(images(s_oth).astype(bf16)).astype(f32)
        chunk = scatter_sum(half.astype(bf16).reshape(8, 64, L), "z")
        i_own = gather(chunk, "z", 8).reshape(512, L)
        i_oth = swap(i_own)
        both = products(s_oth, i_oth, products(s_own, i_own))
        sums = scatter_sum(both, ("x", "y"))
        whole = gather(sums, ("x", "y"), 16)
        if it < ITERS - 1:
            projected = factor_step(whole, False)
    projected, inverse = factor_step(whole, True)
    partial = jnp.sum(projected * projected, axis=0, keepdims=True)
    partial = partial + swap(partial)
    energies = gather(partial, "z", 8)
    rows = jnp.concatenate(
        [lax.dynamic_slice_in_dim(inverse, 8 * ((2 * c + (y + k) % 2) * 8 + z), 8, 0) for k in (0, 1)], axis=0
    )
    own, oth = (
        lax.dot_general(rows, i, (((1,), (1,)), ((), ())), precision=HI, preferred_element_type=f32)
        for i in (i_own, i_oth)
    )
    basis = jnp.where(c == 0, jnp.concatenate([own, oth], axis=1), jnp.concatenate([oth, own], axis=1))
    out = []
    for k in (0, 1):
        pairs = [(2 * v + d, 2 * (2 * d + (v + k) % 2) + v // 2) for v in range(4) for d in range(2)]
        out.append(lax.ppermute(basis[8 * k : 8 * k + 8], ("y", "c"), pairs))
    scalars = jnp.stack([shrink_index[0], y * 8 + z, y % 2]).astype(jnp.int32)
    return finish(scalars, energies, *out)


def solution(mesh):
    grid = Mesh(mesh.devices.reshape(4, 8, 4, 2), ("y", "z", "x", "c"))
    rows, cols = ("y", "z"), ("x", "c")
    return jax.shard_map(
        body,
        mesh=grid,
        in_specs=(P(rows, cols), P(cols, None), P()),
        out_specs=P(rows, cols),
        check_vma=False,
    )
```

```python
import jax
import jax.numpy as jnp
from jax import lax
from jax.experimental import pallas as pl
from jax.experimental.pallas import tpu as pltpu
from jax.sharding import Mesh, PartitionSpec as P

ITERS = 3
f32 = jnp.float32
bf16 = jnp.bfloat16
HI = lax.Precision.HIGHEST
VMEM = pl.BlockSpec(memory_space=pltpu.VMEM)
L = 256
PANEL = 32
LANES = 128


def vmem(shape, dtype=f32):
    return pltpu.VMEM(shape, dtype)


def near(*arrays):
    return tuple(pltpu.with_memory_space_constraint(x, pltpu.VMEM) for x in arrays)


def limit(mib):
    return pltpu.CompilerParams(vmem_limit_bytes=mib << 20)


def tdot(a, b):
    return lax.dot_general(a, b, (((0,), (0,)), ((), ())), precision=HI, preferred_element_type=f32)


def factor_inverse(g_ref, b_ref, w_ref, x_ref):
    sub = lax.broadcasted_iota(jnp.int32, (8, LANES), 0)
    lane = lax.broadcasted_iota(jnp.int32, (8, LANES), 1)
    groups = PANEL // 8
    b_ref[:, 0:L] = g_ref[0:LANES, :]
    b_ref[:, L:] = jnp.zeros((LANES, LANES), f32)

    def half(step, carry):
        for k in range(LANES // PANEL):
            c0 = k * PANEL
            base = b_ref[c0 : c0 + PANEL, :]
            if k > 0:
                base = base - tdot(w_ref[0:c0, c0 : c0 + PANEL], w_ref[0:c0, :])
            a = [[base[8 * q : 8 * q + 8, LANES * t : LANES * (t + 1)] for t in range(3)] for q in range(groups)]
            for q in range(groups):
                a[q][2] = a[q][2] + jnp.where(lane == sub + (c0 + 8 * q), 1.0, 0.0).astype(f32)
            for p in range(0, groups, 2):
                c = c0 + 8 * p
                col = [
                    {q: jnp.broadcast_to(a[q][0][:, c + i : c + i + 1], (8, LANES)) for q in range(p, groups)}
                    for i in range(16)
                ]
                for j in range(16):
                    h, r = p + j // 8, j % 8
                    below = range(h, groups)
                    inv = lax.rsqrt(jnp.broadcast_to(col[j][h][r : r + 1, :], (8, LANES)))
                    m = {q: col[j][q] * inv for q in below}
                    m[h] = jnp.where(sub > r, m[h], 0.0)
                    row = [jnp.broadcast_to(a[h][t][r : r + 1, :], (8, LANES)) * inv for t in range(3)]
                    for i in range(j + 1, 16):
                        ci = jnp.broadcast_to(col[i][h][r : r + 1, :], (8, LANES)) * inv
                        for q in below:
                            col[i][q] = col[i][q] - m[q] * ci
                    for q in below:
                        for t in range(3):
                            a[q][t] = a[q][t] - m[q] * row[t]
                    for t in range(3):
                        a[h][t] = jnp.where(sub == r, row[t], a[h][t])
            for q in range(groups):
                for t in range(3):
                    w_ref[c0 + 8 * q : c0 + 8 * q + 8, LANES * t : LANES * (t + 1)] = a[q][t]

        @pl.when(step == 0)
        def _():
            x_ref[0:LANES, 0:LANES] = w_ref[:, L:]
            x_ref[0:LANES, LANES:L] = jnp.zeros((LANES, LANES), f32)
            u = tdot(w_ref[:, LANES:L], w_ref[:, LANES:])
            b_ref[:, 0:LANES] = g_ref[LANES:L, LANES:L] - u[:, :LANES]
            b_ref[:, LANES:L] = -u[:, LANES:]

        @pl.when(step == 1)
        def _():
            x_ref[LANES:L, :] = w_ref[:, LANES:]

        return carry

    lax.fori_loop(0, 2, half, 0)


def step_kernel(s_ref, p_ref, x_ref, w_ref, b_ref, g_ref):
    for d in range(16):
        r = 8 * d
        g_ref[r : r + 8, 0:LANES] = s_ref[d, 0:8, :]
        g_ref[r : r + 8, LANES:L] = s_ref[d, 8:16, :]
        g_ref[LANES + r : LANES + r + 8, LANES:L] = s_ref[d, 16:24, :]
    factor_inverse(g_ref, b_ref, w_ref, x_ref)
    last = len(p_ref.shape) == 3
    energy = jnp.zeros((1, L), f32)
    for n in range(2):
        halves = [jnp.concatenate([s_ref[8 * n + d, h : h + 32, :] for d in range(8)], axis=0) for h in (24, 56)]
        p = lax.dot_general(
            jnp.concatenate(halves, axis=1), x_ref[...], (((1,), (1,)), ((), ())), precision=HI, preferred_element_type=f32
        )
        if last:
            energy = energy + jnp.sum(p * p, axis=0, keepdims=True)
        else:
            p_ref[256 * n : 256 * n + 256, :] = p.astype(bf16)
    if last:
        for d in range(16):
            p_ref[d] = energy


def factor_step(s, last):
    shared = [vmem((LANES, 3 * LANES)), vmem((LANES, 3 * LANES)), vmem((L, L))]
    inverse = vmem((L, L))
    projected = vmem((16, 1, L)) if last else vmem((512, L), bf16)
    return pl.pallas_call(
        step_kernel,
        out_shape=(projected, inverse) if last else projected,
        in_specs=[VMEM],
        out_specs=(VMEM, VMEM) if last else VMEM,
        scratch_shapes=shared if last else [inverse, *shared],
        compiler_params=limit(12),
        name="factor_step",
    )(*near(s))


def split(v):
    a = v.astype(bf16)
    r = v - a.astype(f32)
    b = r.astype(bf16)
    return a, b, (r - b.astype(f32)).astype(bf16)


def whole_rows(i):
    return jnp.concatenate([i[d] for d in range(8)], axis=0)


def products_kernel(s_ref, i_ref, *refs):
    o_ref = refs[-1]
    i = whole_rows(i_ref)
    t = sum(jnp.dot(s_ref[...], part, preferred_element_type=f32) for part in split(i))
    top = tdot(i[:, :LANES], i)
    low = tdot(i[:, LANES:], i[:, LANES:])
    for d in range(16):
        r, q = slice(8 * d, 8 * d + 8), slice(32 * d, 32 * d + 32)
        both = jnp.concatenate([top[r, :LANES], top[r, LANES:], low[r, :], t[q, :LANES], t[q, LANES:]], axis=0)
        o_ref[d] = both if len(refs) == 1 else both + refs[0][d]


def basis_kernel(r_ref, i_ref, o_ref):
    o_ref[...] = lax.dot_general(
        r_ref[...], whole_rows(i_ref), (((1,), (1,)), ((), ())), precision=HI, preferred_element_type=f32
    )


def basis_rows(rows, i):
    return pl.pallas_call(
        basis_kernel,
        out_shape=vmem((16, 512)),
        in_specs=[VMEM] * 2,
        out_specs=VMEM,
        compiler_params=limit(8),
        name="basis_rows",
    )(*near(rows, i))


def products(s, i, *add):
    return pl.pallas_call(
        products_kernel,
        out_shape=vmem((16, 88, LANES)),
        in_specs=[VMEM] * (2 + len(add)),
        out_specs=VMEM,
        compiler_params=limit(16),
        name="products",
    )(*near(s, i, *add))


def finish_kernel(n_ref, e_ref, a_ref, b_ref, o_ref, t_ref):
    e = e_ref[0]
    for d in range(1, 16):
        e = e + e_ref[d]
    across = jnp.broadcast_to(e, (L, L))
    t_ref[...] = jnp.transpose(across)
    down = t_ref[...]
    k = n_ref[0]
    above = jnp.sum((across > down).astype(jnp.int32), axis=1, keepdims=True)
    least = jnp.sum((across >= down).astype(jnp.int32), axis=1, keepdims=True)
    at_k = (above <= k) & (k < least)
    threshold = jnp.max(jnp.where(at_k, down[:, 0:1], -jnp.inf), axis=0, keepdims=True)
    mine = t_ref[pl.ds(pl.multiple_of(n_ref[1] * 8, 8), 8), 0:1]
    factor = jnp.sqrt(jnp.maximum(mine - threshold, 0.25 * threshold))
    odd = n_ref[2] == 1
    a = a_ref[...] * factor
    b = b_ref[...] * factor
    o_ref[:, 0:1024] = jnp.where(odd, b, a)
    o_ref[:, 1024:2048] = jnp.where(odd, a, b)


def finish(scalars, energies, a, b):
    return pl.pallas_call(
        finish_kernel,
        out_shape=jax.ShapeDtypeStruct((8, 2048), f32),
        in_specs=[pl.BlockSpec(memory_space=pltpu.SMEM)] + [VMEM] * 3,
        out_specs=VMEM,
        scratch_shapes=[pltpu.VMEM((L, L), f32)],
        compiler_params=limit(8),
        name="finish",
    )(scalars, *near(energies, a, b))


def gather(x, axis, n):
    return lax.all_to_all(jnp.broadcast_to(x, (n, *x.shape)), axis, 0, 0, tiled=True)


def scatter_sum(x, axis):
    return jnp.sum(lax.all_to_all(x, axis, 0, 0, tiled=True).astype(f32), axis=0)


def swap(x):
    return lax.ppermute(x, "c", [(0, 1), (1, 0)])


def body(sketches, start_basis, shrink_index):
    y, z, c = lax.axis_index("y"), lax.axis_index("z"), lax.axis_index("c")
    parts = []
    for k in (0, 1):
        half = lax.dynamic_slice_in_dim(sketches, ((y + k) % 2) * 1024, 1024, 1)
        pairs = [(2 * v + d, 2 * (2 * d + (v + k) % 2) + v // 2) for v in range(4) for d in range(2)]
        parts.append(lax.ppermute(half, ("y", "c"), pairs))
    odd = y % 2 == 1
    s = jnp.concatenate([jnp.where(odd, parts[1], parts[0]), jnp.where(odd, parts[0], parts[1])], axis=0)
    s_own = lax.dynamic_slice_in_dim(s, c * 512, 512, 1)
    s_oth = lax.dynamic_slice_in_dim(s, (1 - c) * 512, 512, 1)

    t = jnp.dot(sketches, start_basis, preferred_element_type=f32)
    chunk = scatter_sum(t.reshape(8, 32, L), ("x", "c")).astype(bf16)
    rows = gather(chunk, ("x", "c"), 8).reshape(256, L)
    same = lax.ppermute(rows, ("y", "c"), [(2 * v + d, 2 * (2 * (v % 2) + d) + v // 2) for v in range(4) for d in range(2)])
    flip = lax.ppermute(rows, ("y", "c"), [(2 * v + d, 2 * (2 * (1 - v % 2) + d) + v // 2) for v in range(4) for d in range(2)])
    upper = y // 2 == 1
    projected = jnp.concatenate([jnp.where(upper, flip, same), jnp.where(upper, same, flip)], axis=0)
    for it in range(ITERS):
        def images(part):
            return lax.dot_general(part, projected, (((0,), (0,)), ((), ())), preferred_element_type=f32)

        half = images(s_own) + swap(images(s_oth).astype(bf16)).astype(f32)
        chunk = scatter_sum(half.astype(bf16).reshape(8, 64, L), "z")
        i_own = gather(chunk, "z", 8)
        i_oth = swap(i_own)
        both = products(s_oth, i_oth, products(s_own, i_own))
        sums = scatter_sum(both, ("x", "y"))
        whole = gather(sums, ("x", "y"), 16)
        if it < ITERS - 1:
            projected = factor_step(whole, False)
    partial, inverse = factor_step(whole, True)
    energies = lax.all_to_all(partial, ("z", "c"), 0, 0, tiled=True)
    rows = jnp.concatenate(
        [lax.dynamic_slice_in_dim(inverse, 8 * ((2 * c + (y + k) % 2) * 8 + z), 8, 0) for k in (0, 1)], axis=0
    )
    own, oth = (basis_rows(rows, i) for i in (i_own, i_oth))
    basis = jnp.where(c == 0, jnp.concatenate([own, oth], axis=1), jnp.concatenate([oth, own], axis=1))
    out = []
    for k in (0, 1):
        pairs = [(2 * v + d, 2 * (2 * d + (v + k) % 2) + v // 2) for v in range(4) for d in range(2)]
        out.append(lax.ppermute(basis[8 * k : 8 * k + 8], ("y", "c"), pairs))
    scalars = jnp.stack([shrink_index[0], y * 8 + z, y % 2]).astype(jnp.int32)
    return finish(scalars, energies, *out)


def solution(mesh):
    grid = Mesh(mesh.devices.reshape(4, 8, 4, 2), ("y", "z", "x", "c"))
    rows, cols = ("y", "z"), ("x", "c")
    return jax.shard_map(
        body,
        mesh=grid,
        in_specs=(P(rows, cols), P(cols, None), P()),
        out_specs=P(rows, cols),
        check_vma=False,
    )
```

```python
import jax
import jax.numpy as jnp
from jax import lax
from jax.experimental import pallas as pl
from jax.experimental.pallas import tpu as pltpu
from jax.sharding import Mesh, PartitionSpec as P

ITERS = 3
f32 = jnp.float32
bf16 = jnp.bfloat16
HI = lax.Precision.HIGHEST
VMEM = pl.BlockSpec(memory_space=pltpu.VMEM)
L = 256
PANEL = 32
LANES = 128


def vmem(shape, dtype=f32):
    return pltpu.VMEM(shape, dtype)


def near(*arrays):
    return tuple(pltpu.with_memory_space_constraint(x, pltpu.VMEM) for x in arrays)


def limit(mib):
    return pltpu.CompilerParams(vmem_limit_bytes=mib << 20)


def tdot(a, b):
    return lax.dot_general(a, b, (((0,), (0,)), ((), ())), precision=HI, preferred_element_type=f32)


def factor_inverse(g_ref, b_ref, w_ref, x_ref):
    sub = lax.broadcasted_iota(jnp.int32, (8, LANES), 0)
    lane = lax.broadcasted_iota(jnp.int32, (8, LANES), 1)
    groups = PANEL // 8
    b_ref[:, 0:L] = g_ref[0:LANES, :]
    b_ref[:, L:] = jnp.zeros((LANES, LANES), f32)

    def half(step, carry):
        for k in range(LANES // PANEL):
            c0 = k * PANEL
            base = b_ref[c0 : c0 + PANEL, :]
            if k > 0:
                base = base - tdot(w_ref[0:c0, c0 : c0 + PANEL], w_ref[0:c0, :])
            a = [[base[8 * q : 8 * q + 8, LANES * t : LANES * (t + 1)] for t in range(3)] for q in range(groups)]
            for q in range(groups):
                a[q][2] = a[q][2] + jnp.where(lane == sub + (c0 + 8 * q), 1.0, 0.0).astype(f32)
            for p in range(0, groups, 2):
                c = c0 + 8 * p
                col = [
                    {q: jnp.broadcast_to(a[q][0][:, c + i : c + i + 1], (8, LANES)) for q in range(p, groups)}
                    for i in range(16)
                ]
                for j in range(16):
                    h, r = p + j // 8, j % 8
                    below = range(h, groups)
                    inv = lax.rsqrt(jnp.broadcast_to(col[j][h][r : r + 1, :], (8, LANES)))
                    m = {q: col[j][q] * inv for q in below}
                    m[h] = jnp.where(sub > r, m[h], 0.0)
                    row = [jnp.broadcast_to(a[h][t][r : r + 1, :], (8, LANES)) * inv for t in range(3)]
                    for i in range(j + 1, 16):
                        ci = jnp.broadcast_to(col[i][h][r : r + 1, :], (8, LANES)) * inv
                        for q in below:
                            col[i][q] = col[i][q] - m[q] * ci
                    for q in below:
                        for t in range(3):
                            a[q][t] = a[q][t] - m[q] * row[t]
                    for t in range(3):
                        a[h][t] = jnp.where(sub == r, row[t], a[h][t])
            for q in range(groups):
                for t in range(3):
                    w_ref[c0 + 8 * q : c0 + 8 * q + 8, LANES * t : LANES * (t + 1)] = a[q][t]

        @pl.when(step == 0)
        def _():
            x_ref[0:LANES, 0:LANES] = w_ref[:, L:]
            x_ref[0:LANES, LANES:L] = jnp.zeros((LANES, LANES), f32)
            u = tdot(w_ref[:, LANES:L], w_ref[:, LANES:])
            b_ref[:, 0:LANES] = g_ref[LANES:L, LANES:L] - u[:, :LANES]
            b_ref[:, LANES:L] = -u[:, LANES:]

        @pl.when(step == 1)
        def _():
            x_ref[LANES:L, :] = w_ref[:, LANES:]

        return carry

    lax.fori_loop(0, 2, half, 0)


def step_kernel(s_ref, p_ref, x_ref, w_ref, b_ref, g_ref):
    for d in range(16):
        r = 8 * d
        g_ref[r : r + 8, 0:LANES] = s_ref[d, 0:8, :]
        g_ref[r : r + 8, LANES:L] = s_ref[d, 8:16, :]
        g_ref[LANES + r : LANES + r + 8, LANES:L] = s_ref[d, 16:24, :]
    factor_inverse(g_ref, b_ref, w_ref, x_ref)
    last = len(p_ref.shape) == 3
    energy = jnp.zeros((1, L), f32)
    for n in range(2):
        halves = [jnp.concatenate([s_ref[8 * n + d, h : h + 32, :] for d in range(8)], axis=0) for h in (24, 56)]
        p = lax.dot_general(
            jnp.concatenate(halves, axis=1), x_ref[...], (((1,), (1,)), ((), ())), precision=HI, preferred_element_type=f32
        )
        if last:
            energy = energy + jnp.sum(p * p, axis=0, keepdims=True)
        else:
            p_ref[256 * n : 256 * n + 256, :] = p.astype(bf16)
    if last:
        for d in range(16):
            p_ref[d] = energy


def factor_step(s, last):
    shared = [vmem((LANES, 3 * LANES)), vmem((LANES, 3 * LANES)), vmem((L, L))]
    inverse = vmem((L, L))
    projected = vmem((16, 1, L)) if last else vmem((512, L), bf16)
    return pl.pallas_call(
        step_kernel,
        out_shape=(projected, inverse) if last else projected,
        in_specs=[VMEM],
        out_specs=(VMEM, VMEM) if last else VMEM,
        scratch_shapes=shared if last else [inverse, *shared],
        compiler_params=limit(12),
        name="factor_step",
    )(*near(s))


def split(v):
    a = v.astype(bf16)
    r = v - a.astype(f32)
    b = r.astype(bf16)
    return a, b, (r - b.astype(f32)).astype(bf16)


def whole_rows(i):
    return jnp.concatenate([i[d] for d in range(8)], axis=0)


def products_kernel(s_ref, i_ref, *refs):
    o_ref = refs[-1]
    i = whole_rows(i_ref)
    t = sum(jnp.dot(s_ref[...], part, preferred_element_type=f32) for part in split(i))
    top = tdot(i[:, :LANES], i)
    low = tdot(i[:, LANES:], i[:, LANES:])
    for d in range(16):
        r, q = slice(8 * d, 8 * d + 8), slice(32 * d, 32 * d + 32)
        both = jnp.concatenate([top[r, :LANES], top[r, LANES:], low[r, :], t[q, :LANES], t[q, LANES:]], axis=0)
        o_ref[d] = both if len(refs) == 1 else both + refs[0][d]


def basis_kernel(r_ref, i_ref, o_ref):
    o_ref[...] = lax.dot_general(
        r_ref[...], whole_rows(i_ref), (((1,), (1,)), ((), ())), precision=HI, preferred_element_type=f32
    )


def basis_rows(rows, i):
    return pl.pallas_call(
        basis_kernel,
        out_shape=vmem((16, 512)),
        in_specs=[VMEM] * 2,
        out_specs=VMEM,
        compiler_params=limit(8),
        name="basis_rows",
    )(*near(rows, i))


def products(s, i, *add):
    return pl.pallas_call(
        products_kernel,
        out_shape=vmem((16, 88, LANES)),
        in_specs=[VMEM] * (2 + len(add)),
        out_specs=VMEM,
        compiler_params=limit(16),
        name="products",
    )(*near(s, i, *add))


def finish_kernel(n_ref, e_ref, a_ref, b_ref, o_ref, t_ref):
    e = e_ref[0]
    for d in range(1, 16):
        e = e + e_ref[d]
    across = jnp.broadcast_to(e, (L, L))
    t_ref[...] = jnp.transpose(across)
    down = t_ref[...]
    k = n_ref[0]
    above = jnp.sum((across > down).astype(jnp.int32), axis=1, keepdims=True)
    least = jnp.sum((across >= down).astype(jnp.int32), axis=1, keepdims=True)
    at_k = (above <= k) & (k < least)
    threshold = jnp.max(jnp.where(at_k, down[:, 0:1], -jnp.inf), axis=0, keepdims=True)
    mine = t_ref[pl.ds(pl.multiple_of(n_ref[1] * 8, 8), 8), 0:1]
    factor = jnp.sqrt(jnp.maximum(mine - threshold, 0.25 * threshold))
    odd = n_ref[2] == 1
    a = a_ref[...] * factor
    b = b_ref[...] * factor
    o_ref[:, 0:1024] = jnp.where(odd, b, a)
    o_ref[:, 1024:2048] = jnp.where(odd, a, b)


def finish(scalars, energies, a, b):
    return pl.pallas_call(
        finish_kernel,
        out_shape=jax.ShapeDtypeStruct((8, 2048), f32),
        in_specs=[pl.BlockSpec(memory_space=pltpu.SMEM)] + [VMEM] * 3,
        out_specs=VMEM,
        scratch_shapes=[pltpu.VMEM((L, L), f32)],
        compiler_params=limit(8),
        name="finish",
    )(scalars, *near(energies, a, b))


def gather(x, axis, n):
    return lax.all_to_all(jnp.broadcast_to(x, (n, *x.shape)), axis, 0, 0, tiled=True)


def scatter_sum(x, axis):
    return jnp.sum(lax.all_to_all(x, axis, 0, 0, tiled=True).astype(f32), axis=0)


def swap(x):
    return lax.ppermute(x, "c", [(0, 1), (1, 0)])


def body(sketches, start_basis, shrink_index):
    y, z, c = lax.axis_index("y"), lax.axis_index("z"), lax.axis_index("c")
    parts = []
    for k in (0, 1):
        half = lax.dynamic_slice_in_dim(sketches, ((y + k) % 2) * 1024, 1024, 1)
        pairs = [(2 * v + d, 2 * (2 * d + (v + k) % 2) + v // 2) for v in range(4) for d in range(2)]
        parts.append(lax.ppermute(half, ("y", "c"), pairs))
    odd = y % 2 == 1
    s = jnp.concatenate([jnp.where(odd, parts[1], parts[0]), jnp.where(odd, parts[0], parts[1])], axis=0)
    s_own = lax.dynamic_slice_in_dim(s, c * 512, 512, 1)
    s_oth = lax.dynamic_slice_in_dim(s, (1 - c) * 512, 512, 1)

    t = jnp.dot(sketches, start_basis, preferred_element_type=f32)
    chunk = scatter_sum(t.reshape(8, 32, L), ("x", "c")).astype(bf16)
    rows = gather(chunk, ("x", "c"), 8).reshape(256, L)
    same = lax.ppermute(rows, ("y", "c"), [(2 * v + d, 2 * (2 * (v % 2) + d) + v // 2) for v in range(4) for d in range(2)])
    flip = lax.ppermute(rows, ("y", "c"), [(2 * v + d, 2 * (2 * (1 - v % 2) + d) + v // 2) for v in range(4) for d in range(2)])
    upper = y // 2 == 1
    projected = jnp.concatenate([jnp.where(upper, flip, same), jnp.where(upper, same, flip)], axis=0)
    for it in range(ITERS):
        def images(part):
            return lax.dot_general(part, projected, (((0,), (0,)), ((), ())), preferred_element_type=f32)

        sent = swap(images(s_oth).astype(bf16))
        half = lax.optimization_barrier(images(s_own)) + sent.astype(f32)
        chunk = scatter_sum(half.astype(bf16).reshape(8, 64, L), "z")
        i_own = gather(chunk, "z", 8)
        i_oth = swap(i_own)
        both = products(s_oth, i_oth, products(s_own, i_own))
        sums = scatter_sum(both, ("x", "y"))
        whole = gather(sums, ("x", "y"), 16)
        if it < ITERS - 1:
            projected = factor_step(whole, False)
    partial, inverse = factor_step(whole, True)
    energies = lax.all_to_all(partial, ("z", "c"), 0, 0, tiled=True)
    rows = jnp.concatenate(
        [lax.dynamic_slice_in_dim(inverse, 8 * ((2 * c + (y + k) % 2) * 8 + z), 8, 0) for k in (0, 1)], axis=0
    )
    own, oth = (basis_rows(rows, i) for i in (i_own, i_oth))
    basis = jnp.where(c == 0, jnp.concatenate([own, oth], axis=1), jnp.concatenate([oth, own], axis=1))
    out = []
    for k in (0, 1):
        pairs = [(2 * v + d, 2 * (2 * d + (v + k) % 2) + v // 2) for v in range(4) for d in range(2)]
        out.append(lax.ppermute(basis[8 * k : 8 * k + 8], ("y", "c"), pairs))
    scalars = jnp.stack([shrink_index[0], y * 8 + z, y % 2]).astype(jnp.int32)
    return finish(scalars, energies, *out)


def solution(mesh):
    grid = Mesh(mesh.devices.reshape(4, 8, 4, 2), ("y", "z", "x", "c"))
    rows, cols = ("y", "z"), ("x", "c")
    return jax.shard_map(
        body,
        mesh=grid,
        in_specs=(P(rows, cols), P(cols, None), P()),
        out_specs=P(rows, cols),
        check_vma=False,
    )
```
